256 devices in a mesh: seq: 256 (over x, y, z, core).
Axes of the slice: x: 4, y: 4, z: 8, core: 2. Of those that a mesh axis runs over, the one named last changes fastest.
Arguments:
- tokens: bfloat16 [131072, 1024], P('seq'), may hold values from -128 to 128, as said below
- w_query: bfloat16 [1024, 1024], replicated, may hold values from -0.1875 to 0.1875
- w_key: bfloat16 [1024, 256], replicated, may hold values from -0.1875 to 0.1875
- w_value: bfloat16 [1024, 256], replicated, may hold values from -0.1875 to 0.1875
- w_out: bfloat16 [1024, 1024], replicated, may hold values from -0.1875 to 0.1875
Outputs:
- attended: bfloat16 [131072, 1024], P('seq')
The draws below stay inside these ranges and needn't reach their ends.
Inputs may be any that keep to these rules, and one draw needn't show every extreme that they name: `tokens`: Real-valued activations.
All inputs are finite; a program needn't handle non-finite values.
Results may differ from the reference program's by a relative error of at most 0.007.
The reference program's roundings to bfloat16 on the way (of `queries`, `key_rows`, `value_rows`, `middle`, `coarse`, `probabilities` and `mixed`) count: a program that leaves them out, or rounds other values in their place, can miss the bound.
Values may be sent and summed in bfloat16 or wider, within the bound.
A program may use at most 128 MiB of HBM per device.

```python
import math
import jax
import jax.numpy as jnp
from jax import lax

D = 1024
HEADS = 16
KV_HEADS = 4
HEAD_DIM = 64
BLOCK = 256
POOL = 16
GROUP = 16
TOK_DEV = 512
SEQ = 131072


def draw_tokens(key, part):
    block_total = SEQ // BLOCK
    run_total = SEQ // POOL
    block_vectors = jnp.clip(jax.random.normal(jax.random.fold_in(key, 21), (block_total, D), jnp.float32), -6.0, 6.0)
    run_vectors = jnp.clip(jax.random.normal(jax.random.fold_in(key, 22), (run_total, D), jnp.float32), -6.0, 6.0)
    noise_rows = jnp.clip(jax.random.normal(jax.random.fold_in(key, 11), (SEQ, D), jnp.float32), -6.0, 6.0)
    sample_rows = 0.45 * noise_rows.reshape(run_total, POOL, D) + 0.4 * run_vectors[:, None, :]
    sample_rows = sample_rows.reshape(block_total, BLOCK, D) + 0.8 * block_vectors[:, None, :]
    sample_rows = 1.6 * sample_rows
    sample_rows = jnp.clip(sample_rows.reshape(SEQ, D), -128.0, 128.0)
    return sample_rows.astype(jnp.bfloat16)


def centred(rng, shape, scale, bound, held_as=jnp.bfloat16):
    return jnp.clip(scale * jax.random.normal(rng, shape, jnp.float32), -bound, bound).astype(held_as)


def setup_inputs(seed: int = 0) -> dict:
    seeds = jax.random.split(jax.random.key(seed), 6)
    tokens = draw_tokens(jax.random.fold_in(seeds[5], 71), 0)
    w_query = centred(seeds[1], (D, HEADS * HEAD_DIM), D ** -0.5, 0.1875)
    w_key = centred(seeds[2], (D, KV_HEADS * HEAD_DIM), D ** -0.5, 0.1875)
    w_value = centred(seeds[3], (D, KV_HEADS * HEAD_DIM), D ** -0.5, 0.1875)
    w_out = centred(seeds[4], (HEADS * HEAD_DIM, D), (HEADS * HEAD_DIM) ** -0.5, 0.1875)
    return dict(tokens=tokens, w_query=w_query, w_key=w_key, w_value=w_value, w_out=w_out)


def pool_rows(source, factor):
    width = source.shape[-1]
    grouped = source.astype(jnp.float32).reshape(-1, factor, width)
    return lax.optimization_barrier(jnp.mean(grouped, axis=1)).astype(jnp.bfloat16)

def usable_rows(block_index, my_group, all_blocks, group_tokens, group_summaries):
    near = block_index - 1 + jnp.arange(3 * BLOCK, dtype=jnp.int32) // BLOCK
    near_usable = (near >= 0) & (near < all_blocks)
    middle_blocks = (my_group * group_summaries + jnp.arange(group_summaries, dtype=jnp.int32)) * POOL // BLOCK
    middle_usable = jnp.abs(middle_blocks - block_index) > 1
    coarse_blocks = jnp.arange(all_blocks, dtype=jnp.int32)
    coarse_usable = (coarse_blocks * BLOCK // group_tokens != my_group) & (jnp.abs(coarse_blocks - block_index) > 1)
    return jnp.concatenate([near_usable, middle_usable, coarse_usable])

def attend_block(queries, pair_rows, usable):
    span_rows = pair_rows.shape[0]
    key_width = KV_HEADS * HEAD_DIM
    key_rows = pair_rows[:, :key_width].reshape(span_rows, KV_HEADS, HEAD_DIM).astype(jnp.float32)
    value_rows = pair_rows[:, key_width:].reshape(span_rows, KV_HEADS, HEAD_DIM).astype(jnp.float32)
    shaped = queries.reshape(-1, KV_HEADS, HEADS // KV_HEADS, HEAD_DIM).astype(jnp.float32)
    scores = jnp.einsum('qkgd,lkd->kgql', shaped, key_rows) * (1.0 / math.sqrt(HEAD_DIM))
    scores = jnp.where(usable, scores, -1e+30)
    highest = lax.optimization_barrier(jnp.max(scores, axis=-1, keepdims=True))
    weights = jnp.where(usable, jnp.exp(scores - highest), 0.0)
    totals = lax.optimization_barrier(jnp.sum(weights, axis=-1))
    probabilities = weights.astype(jnp.bfloat16)
    weighted = jnp.einsum('kgql,lkd->qkgd', probabilities.astype(jnp.float32), value_rows)
    weighted = weighted / jnp.transpose(totals, (2, 0, 1))[..., None]
    return weighted.reshape(queries.shape[0], HEADS * HEAD_DIM).astype(jnp.bfloat16)

def reference(tokens, w_query, w_key, w_value, w_out):
    queries = jnp.dot(tokens, w_query, preferred_element_type=jnp.float32).astype(jnp.bfloat16)
    key_rows = jnp.dot(tokens, w_key, preferred_element_type=jnp.float32).astype(jnp.bfloat16)
    value_rows = jnp.dot(tokens, w_value, preferred_element_type=jnp.float32).astype(jnp.bfloat16)
    pair_rows = jnp.concatenate([key_rows, value_rows], axis=1)
    middle = pool_rows(pair_rows, POOL)
    coarse = pool_rows(pair_rows, BLOCK)
    all_blocks = SEQ // BLOCK
    group_tokens = GROUP * TOK_DEV
    group_summaries = group_tokens // POOL
    padded = jnp.pad(pair_rows, ((BLOCK, BLOCK), (0, 0)))

    def per_block(block_index):
        my_group = block_index * BLOCK // group_tokens
        near_rows = lax.dynamic_slice_in_dim(padded, (block_index * BLOCK).astype(jnp.int32), 3 * BLOCK, 0)
        group_mid = lax.dynamic_slice_in_dim(middle, (my_group * group_summaries).astype(jnp.int32), group_summaries, 0)
        block_queries = lax.dynamic_slice_in_dim(queries, (block_index * BLOCK).astype(jnp.int32), BLOCK, 0)
        gathered = jnp.concatenate([near_rows, group_mid, coarse], axis=0)
        usable = usable_rows(block_index, my_group, all_blocks, group_tokens, group_summaries)
        return attend_block(block_queries, gathered, usable)
    mixed = lax.map(per_block, jnp.arange(all_blocks, dtype=jnp.int32)).reshape(SEQ, HEADS * HEAD_DIM)
    return jnp.dot(mixed, w_out, preferred_element_type=jnp.float32).astype(jnp.bfloat16)
```

```python
import functools
import math

import jax
import jax.numpy as jnp
from jax import lax
from jax.experimental import pallas as pl
from jax.experimental.pallas import tpu as pltpu
from jax.sharding import PartitionSpec as P

HEADS = 16
KV_HEADS = 4
PER_KV = HEADS // KV_HEADS
HEAD_DIM = 64
BLOCK = 256
POOL = 16
GROUP = 16
CHIPS = GROUP // 2
COLUMNS = 16
TOK = 512
D = 1024
KVW = KV_HEADS * HEAD_DIM
NEAR = 3 * BLOCK
MID = 512
COARSE = 512
VROWS = HEAD_DIM + 16
C_EXP = math.log2(math.e) / math.sqrt(HEAD_DIM)
F32 = jnp.float32
BF16 = jnp.bfloat16
MESH = pl.DeviceIdType.MESH


def iota(shape, dim):
    return lax.broadcasted_iota(jnp.int32, shape, dim)


def dot(a, b):
    return jnp.dot(a, b, preferred_element_type=F32)


def kernel(devices, tok_hbm, wq_hbm, wk_hbm, wv_hbm, wo_hbm, out_ref,
           tok, wkv, wq, wo, near, mid, zc, zf, coarse, qt, kp, vt, acc, mx, mixt,
           load_sem, halo_s, halo_r, mid_s, mid_r, zc_s, zc_r, co_s, co_r, rel_s, rel_r):
    me = lax.axis_index("seq")
    core = lax.rem(me, 2)
    pos = lax.rem(me, GROUP)
    chip = lax.div(pos, 2)
    column = lax.div(me, GROUP)
    all_blocks = devices * 2

    def at(index):
        return (index,)

    loads = [
        pltpu.make_async_copy(tok_hbm, tok, load_sem.at[0]),
        pltpu.make_async_copy(wk_hbm, wkv.at[:, pl.ds(0, KVW)], load_sem.at[1]),
        pltpu.make_async_copy(wv_hbm, wkv.at[:, pl.ds(KVW, KVW)], load_sem.at[2]),
        pltpu.make_async_copy(wq_hbm, wq, load_sem.at[3]),
        pltpu.make_async_copy(wo_hbm, wo, load_sem.at[4]),
    ]
    for copy in loads:
        copy.start()

    def in_column(k):
        return column * GROUP + lax.rem(pos + k, GROUP)

    def across(k):
        return lax.rem(column + k, COLUMNS) * GROUP + pos

    following = lax.rem(me + 1, devices)
    previous = lax.rem(me + devices - 1, devices)
    partner = column * GROUP + chip * 2 + 1 - core

    barrier = pltpu.get_barrier_semaphore()

    def greet(k, _):
        pl.semaphore_signal(barrier, inc=1, device_id=at(in_column(k)), device_id_type=MESH)
        pl.semaphore_signal(barrier, inc=1, device_id=at(across(k)), device_id_type=MESH)
        return 0

    lax.fori_loop(1, GROUP, greet, 0)
    pl.semaphore_signal(barrier, inc=1, device_id=at(following), device_id_type=MESH)
    pl.semaphore_signal(barrier, inc=1, device_id=at(previous), device_id_type=MESH)

    for copy in loads[:3]:
        copy.wait()
    kv = dot(tok[...], wkv[...]).astype(BF16)
    near[pl.ds(BLOCK, TOK), :] = kv

    row, col = iota((32, TOK), 0), iota((32, TOK), 1)
    pool_mid = jnp.where(col // POOL == row, 1.0 / POOL, 0.0).astype(BF16)
    mid[core, chip] = dot(pool_mid, kv).astype(BF16)
    row, col = iota((16, TOK), 0), iota((16, TOK), 1)
    mine = jnp.zeros((16, 128), F32)
    for j in range(4):
        pool_coarse = jnp.where(col // BLOCK == row - 2 * j, 1.0 / BLOCK, 0.0).astype(BF16)
        mine += dot(pool_coarse, kv[:, j * 128:(j + 1) * 128])
    zc[pos] = mine[:8].astype(BF16)

    pl.semaphore_wait(barrier, 2 * GROUP)

    def zc_copy(k):
        return pltpu.make_async_remote_copy(
            src_ref=zc.at[pos], dst_ref=zc.at[pos], send_sem=zc_s.at[k], recv_sem=zc_r.at[k],
            device_id=at(in_column(k)), device_id_type=MESH)

    def halo_copy(which):
        src = near.at[pl.ds((2 - which) * BLOCK, BLOCK), :]
        dst = near.at[pl.ds(which * 3 * BLOCK, BLOCK), :]
        return pltpu.make_async_remote_copy(
            src_ref=src, dst_ref=dst, send_sem=halo_s.at[which], recv_sem=halo_r.at[which],
            device_id=at(previous if which else following), device_id_type=MESH)

    def mid_copy(k):
        target = column * GROUP + lax.rem(chip + k, CHIPS) * 2 + core
        return pltpu.make_async_remote_copy(
            src_ref=mid.at[core, chip], dst_ref=mid.at[core, chip],
            send_sem=mid_s.at[k], recv_sem=mid_r.at[k],
            device_id=at(target), device_id_type=MESH)

    def coarse_copy(k):
        return pltpu.make_async_remote_copy(
            src_ref=coarse.at[column], dst_ref=coarse.at[column],
            send_sem=co_s.at[k], recv_sem=co_r.at[k],
            device_id=at(across(k)), device_id_type=MESH)

    def each(copy_of, count, act):
        def step(k, _):
            getattr(copy_of(k), act)()
            return 0
        lax.fori_loop(1, count, step, 0)

    relay = pltpu.make_async_remote_copy(
        src_ref=mid.at[core], dst_ref=mid.at[core], send_sem=rel_s, recv_sem=rel_r,
        device_id=at(partner), device_id_type=MESH)

    each(zc_copy, GROUP, "start")
    halo_copy(0).start()
    halo_copy(1).start()
    each(mid_copy, CHIPS, "start")

    loads[3].wait()
    q = dot(tok[...], wq[...]).astype(BF16)
    for b in range(2):
        qt[b] = q[b * BLOCK:(b + 1) * BLOCK].T.reshape(HEADS, HEAD_DIM, BLOCK)

    def prepare(b, rows, span, usable):
        own = near[pl.ds(pl.multiple_of(BLOCK + b * BLOCK, BLOCK), 16), :][0:1, :KVW].astype(F32)
        ok_rows = usable(iota((span, 1), 0))
        ok_cols = usable(iota((1, span), 1))
        keys = jnp.where(ok_rows, rows[:, :KVW].astype(F32), own).astype(BF16)
        values = rows[:, KVW:].T.astype(F32)
        values = jnp.where(ok_cols, values, 0.0).astype(BF16)
        count = jnp.broadcast_to(jnp.where(ok_cols, 1.0, 0.0), (16, span)).astype(BF16)
        for kv_head in range(KV_HEADS):
            part = slice(kv_head * HEAD_DIM, (kv_head + 1) * HEAD_DIM)
            kp[kv_head, 0:span, :] = keys[:, part]
            vt[kv_head, 0:HEAD_DIM, 0:span] = values[part]
            vt[kv_head, HEAD_DIM:VROWS, 0:span] = count

    def attend(b, span, first, last):
        def per_kv(kv_head, _):
            keys = kp[kv_head, 0:span, :]
            values = vt[kv_head, :, 0:span]
            for g in range(PER_KV):
                h = kv_head * PER_KV + g
                scores = dot(keys, qt[b, h])
                highest = jnp.max(scores, axis=0, keepdims=True)
                if not first:
                    before = mx[b, h]
                    highest = jnp.maximum(highest, before)
                weights = jnp.exp2((scores - highest) * C_EXP).astype(BF16)
                total = dot(values, weights)
                if not first:
                    total += acc[b, h] * jnp.exp2((before - highest) * C_EXP)
                if last:
                    inverse = 1.0 / total[HEAD_DIM:HEAD_DIM + 1]
                    mixt[b, h] = (total[:HEAD_DIM] * inverse).astype(BF16)
                else:
                    acc[b, h] = total
                    mx[b, h] = highest
            return 0
        lax.fori_loop(0, KV_HEADS, per_kv, 0)

    def near_phase(b):
        block = me * 2 + b
        def usable(i):
            there = block - 1 + i // BLOCK
            return (there >= 0) & (there < all_blocks)
        start = pl.multiple_of(b * BLOCK, BLOCK)
        prepare(b, near[pl.ds(start, NEAR), :], NEAR, usable)
        attend(b, NEAR, True, False)

    def halo_wait(slot):
        pltpu.make_async_remote_copy(
            src_ref=near.at[pl.ds(BLOCK, BLOCK), :],
            dst_ref=near.at[pl.ds(pl.multiple_of(slot * 3 * BLOCK, BLOCK), BLOCK), :],
            send_sem=halo_s.at[slot], recv_sem=halo_r.at[slot],
            device_id=at(following), device_id_type=MESH).wait_recv()

    early = 1 - core
    halo_wait(early)
    near_phase(early)

    each(zc_copy, GROUP, "wait_recv")
    zf[...] = zc[...].astype(F32).reshape(GROUP * 8, 128)
    for r in range(2):
        for j in range(4):
            coarse[column, r * 16:(r + 1) * 16, j * 128:(j + 1) * 128] = (
                zf[pl.ds(2 * j + r, GROUP, stride=8), :].astype(BF16))
    each(coarse_copy, COLUMNS, "start")

    halo_wait(core)
    near_phase(core)

    each(mid_copy, CHIPS, "wait_recv")
    relay.start()
    relay.wait_recv()

    def mid_phase(b, _):
        block = me * 2 + b
        def usable(i):
            there = column * 32 + (i // 32 % CHIPS * 2 + i // 256) * 2 + i // POOL % 2
            return jnp.abs(there - block) > 1
        prepare(b, mid[...].reshape(MID, 2 * KVW), MID, usable)
        attend(b, MID, False, False)
        return 0

    lax.fori_loop(0, 2, mid_phase, 0)

    each(coarse_copy, COLUMNS, "wait_recv")
    loads[4].wait()

    def coarse_phase(b, _):
        block = me * 2 + b
        def usable(i):
            there = i // 32 * 32 + i % 16 * 2 + i // 16 % 2
            return (i // 32 != column) & (jnp.abs(there - block) > 1)
        prepare(b, coarse[...].reshape(COARSE, 2 * KVW), COARSE, usable)
        attend(b, COARSE, False, True)
        mixed = mixt[b].reshape(HEADS * HEAD_DIM, BLOCK).T
        out_ref[pl.ds(pl.multiple_of(b * BLOCK, BLOCK), BLOCK), :] = dot(mixed, wo[...]).astype(BF16)
        return 0

    lax.fori_loop(0, 2, coarse_phase, 0)

    each(zc_copy, GROUP, "wait_send")
    halo_copy(0).wait_send()
    halo_copy(1).wait_send()
    each(mid_copy, CHIPS, "wait_send")
    each(coarse_copy, COLUMNS, "wait_send")
    relay.wait_send()


def body(tokens, w_query, w_key, w_value, w_out):
    devices = lax.axis_size("seq")
    dma = pltpu.SemaphoreType.DMA
    return pl.pallas_call(
        functools.partial(kernel, devices),
        out_shape=jax.ShapeDtypeStruct((TOK, D), BF16),
        in_specs=[pl.BlockSpec(memory_space=pl.ANY)] * 5,
        out_specs=pl.BlockSpec(memory_space=pltpu.VMEM),
        scratch_shapes=[
            pltpu.VMEM((TOK, D), BF16),
            pltpu.VMEM((D, 2 * KVW), BF16),
            pltpu.VMEM((D, HEADS * HEAD_DIM), BF16),
            pltpu.VMEM((HEADS * HEAD_DIM, D), BF16),
            pltpu.VMEM((4 * BLOCK, 2 * KVW), BF16),
            pltpu.VMEM((2, CHIPS, TOK // POOL, 2 * KVW), BF16),
            pltpu.VMEM((GROUP, 8, 128), BF16),
            pltpu.VMEM((GROUP * 8, 128), F32),
            pltpu.VMEM((COLUMNS, 32, 2 * KVW), BF16),
            pltpu.VMEM((2, HEADS, HEAD_DIM, BLOCK), BF16),
            pltpu.VMEM((KV_HEADS, NEAR, HEAD_DIM), BF16),
            pltpu.VMEM((KV_HEADS, VROWS, NEAR), BF16),
            pltpu.VMEM((2, HEADS, VROWS, BLOCK), F32),
            pltpu.VMEM((2, HEADS, 1, BLOCK), F32),
            pltpu.VMEM((2, HEADS, HEAD_DIM, BLOCK), BF16),
            dma((5,)),
            dma((2,)), dma((2,)),
            dma((CHIPS,)), dma((CHIPS,)),
            dma((GROUP,)), dma((GROUP,)),
            dma((COLUMNS,)), dma((COLUMNS,)),
            dma, dma,
        ],
        compiler_params=pltpu.CompilerParams(
            collective_id=0, has_side_effects=True, vmem_limit_bytes=60 * 1024 * 1024),
    )(tokens, w_query, w_key, w_value, w_out)


def solution(mesh):
    placed = (P("seq", None), P(), P(), P(), P())
    return jax.shard_map(
        body, mesh=mesh, in_specs=placed, out_specs=P("seq", None), check_vma=False
    )
```

```python
import functools
import math

import jax
import jax.numpy as jnp
from jax import lax
from jax.experimental import pallas as pl
from jax.experimental.pallas import tpu as pltpu
from jax.sharding import PartitionSpec as P

HEADS = 16
KV_HEADS = 4
PER_KV = HEADS // KV_HEADS
HEAD_DIM = 64
BLOCK = 256
POOL = 16
GROUP = 16
CHIPS = GROUP // 2
COLUMNS = 16
TOK = 512
UNROLL = 8
PIECE = 128
D = 1024
KVW = KV_HEADS * HEAD_DIM
NEAR = 3 * BLOCK
MID = 512
COARSE = 512
VROWS = HEAD_DIM + 16
C_EXP = math.log2(math.e) / math.sqrt(HEAD_DIM)
F32 = jnp.float32
BF16 = jnp.bfloat16
MESH = pl.DeviceIdType.MESH


def iota(shape, dim):
    return lax.broadcasted_iota(jnp.int32, shape, dim)


def dot(a, b):
    return jnp.dot(a, b, preferred_element_type=F32)


def kernel(devices, tok_hbm, wq_hbm, wk_hbm, wv_hbm, out_ref,
           tok, wkv, wq, near, mid, zc, zf, coarse, qt, kp, vt, s0, s1, acc, mx, mixt,
           load_sem, halo_s, halo_r, mid_s, mid_r, zc_s, zc_r, co_s, co_r, rel_s, rel_r):
    me = lax.axis_index("seq")
    core = lax.rem(me, 2)
    pos = lax.rem(me, GROUP)
    chip = lax.div(pos, 2)
    column = lax.div(me, GROUP)
    all_blocks = devices * 2

    def at(index):
        return (index,)

    loads = [
        pltpu.make_async_copy(tok_hbm, tok, load_sem.at[0]),
        pltpu.make_async_copy(wk_hbm, wkv.at[:, pl.ds(0, KVW)], load_sem.at[1]),
        pltpu.make_async_copy(wv_hbm, wkv.at[:, pl.ds(KVW, KVW)], load_sem.at[2]),
        pltpu.make_async_copy(wq_hbm, wq, load_sem.at[3]),
    ]
    for copy in loads:
        copy.start()

    def in_column(k):
        return column * GROUP + lax.rem(pos + k, GROUP)

    def across(k):
        return lax.rem(column + k, COLUMNS) * GROUP + pos

    following = lax.rem(me + 1, devices)
    previous = lax.rem(me + devices - 1, devices)
    partner = column * GROUP + chip * 2 + 1 - core

    barrier = pltpu.get_barrier_semaphore()

    def greet(k, _):
        pl.semaphore_signal(barrier, inc=1, device_id=at(in_column(k)), device_id_type=MESH)
        pl.semaphore_signal(barrier, inc=1, device_id=at(across(k)), device_id_type=MESH)
        return 0

    lax.fori_loop(1, GROUP, greet, 0)
    pl.semaphore_signal(barrier, inc=1, device_id=at(following), device_id_type=MESH)
    pl.semaphore_signal(barrier, inc=1, device_id=at(previous), device_id_type=MESH)

    for copy in loads[:3]:
        copy.wait()
    kv = dot(tok[...], wkv[...]).astype(BF16)
    near[pl.ds(BLOCK, TOK), :] = kv

    row, col = iota((32, TOK), 0), iota((32, TOK), 1)
    pool_mid = jnp.where(col // POOL == row, 1.0 / POOL, 0.0).astype(BF16)
    mid[core, chip] = dot(pool_mid, kv).astype(BF16)
    row, col = iota((16, TOK), 0), iota((16, TOK), 1)
    mine = jnp.zeros((16, 128), F32)
    for j in range(4):
        pool_coarse = jnp.where(col // BLOCK == row - 2 * j, 1.0 / BLOCK, 0.0).astype(BF16)
        mine += dot(pool_coarse, kv[:, j * 128:(j + 1) * 128])
    zc[pos] = mine[:8].astype(BF16)

    pl.semaphore_wait(barrier, 2 * GROUP)

    def zc_copy(k):
        return pltpu.make_async_remote_copy(
            src_ref=zc.at[pos], dst_ref=zc.at[pos], send_sem=zc_s.at[k], recv_sem=zc_r.at[k],
            device_id=at(in_column(k)), device_id_type=MESH)

    def halo_copy(which):
        src = near.at[pl.ds((2 - which) * BLOCK, BLOCK), :]
        dst = near.at[pl.ds(which * 3 * BLOCK, BLOCK), :]
        return pltpu.make_async_remote_copy(
            src_ref=src, dst_ref=dst, send_sem=halo_s.at[which], recv_sem=halo_r.at[which],
            device_id=at(previous if which else following), device_id_type=MESH)

    def mid_copy(k):
        target = column * GROUP + lax.rem(chip + k, CHIPS) * 2 + core
        return pltpu.make_async_remote_copy(
            src_ref=mid.at[core, chip], dst_ref=mid.at[core, chip],
            send_sem=mid_s.at[k], recv_sem=mid_r.at[k],
            device_id=at(target), device_id_type=MESH)

    def coarse_copy(k):
        return pltpu.make_async_remote_copy(
            src_ref=coarse.at[column], dst_ref=coarse.at[column],
            send_sem=co_s.at[k], recv_sem=co_r.at[k],
            device_id=at(across(k)), device_id_type=MESH)

    def each(copy_of, count, act):
        def step(k, _):
            getattr(copy_of(k), act)()
            return 0
        lax.fori_loop(1, count, step, 0)

    relay = pltpu.make_async_remote_copy(
        src_ref=mid.at[core], dst_ref=mid.at[core], send_sem=rel_s, recv_sem=rel_r,
        device_id=at(partner), device_id_type=MESH)

    each(zc_copy, GROUP, "start")
    halo_copy(0).start()
    halo_copy(1).start()
    each(mid_copy, CHIPS, "start")

    loads[3].wait()
    q = dot(tok[...], wq[...]).astype(BF16)
    for b in range(2):
        qt[b] = q[b * BLOCK:(b + 1) * BLOCK].T.reshape(HEADS, HEAD_DIM, BLOCK)

    def prepare(at_row, span, rows_at, variants):
        for r in range(0, span, PIECE):
            rows = rows_at(r)
            keys, values = rows[:, :KVW], rows[:, KVW:].T
            for slot, usable, own in variants:
                slot_keys, slot_values, count = keys, values, jnp.ones((16, PIECE), BF16)
                if usable is not None:
                    ok_rows = usable(iota((PIECE, 1), 0) + r)
                    ok_cols = usable(iota((1, PIECE), 1) + r)
                    slot_keys = jnp.where(ok_rows, keys.astype(F32), own).astype(BF16)
                    slot_values = jnp.where(ok_cols, values.astype(F32), 0.0).astype(BF16)
                    count = jnp.broadcast_to(jnp.where(ok_cols, 1.0, 0.0), (16, PIECE)).astype(BF16)
                there = pl.ds(at_row + r, PIECE)
                for kv_head in range(KV_HEADS):
                    part = slice(kv_head * HEAD_DIM, (kv_head + 1) * HEAD_DIM)
                    kp[slot, kv_head, there, :] = slot_keys[:, part]
                    vt[slot, kv_head, 0:HEAD_DIM, there] = slot_values[part]
                    vt[slot, kv_head, HEAD_DIM:VROWS, there] = count

    def own_key(b):
        return near[BLOCK + b * BLOCK:BLOCK + b * BLOCK + 16, :KVW].astype(F32)[0:1]

    def attend(base, span, shared, first, last):
        items = 2 * HEADS

        def place(i):
            b, h = lax.div(i, HEADS), lax.rem(i, HEADS)
            return b, h, (0 if shared else b), lax.div(h, PER_KV)

        def step(ahead, s_ahead, now, s_now, highest):
            if ahead is not None:
                b, h, slot, kv_head = place(ahead)
                query = qt[b, h]
                top = None
            if now is not None:
                nb, nh, nslot, nkv = place(now)
                total = None
            for t in range(0, span, BLOCK):
                if ahead is not None:
                    scores = dot(kp[slot, kv_head, base + t:base + t + BLOCK, :], query)
                    s_ahead[t:t + BLOCK, :] = scores
                    peak = jnp.max(scores.reshape(BLOCK // 8, 8, BLOCK), axis=0)
                    top = peak if top is None else jnp.maximum(top, peak)
                if now is not None:
                    weights = jnp.exp2((s_now[t:t + BLOCK, :] - highest) * C_EXP).astype(BF16)
                    part = dot(vt[nslot, nkv, :, base + t:base + t + BLOCK], weights)
                    total = part if total is None else total + part
            if now is not None:
                if not first:
                    total += acc[nb, nh] * jnp.exp2((mx[nb, nh] - highest) * C_EXP)
                if last:
                    inverse = 1.0 / total[HEAD_DIM:HEAD_DIM + 1]
                    mixt[nb, nh] = (total[:HEAD_DIM] * inverse).astype(BF16)
                else:
                    acc[nb, nh] = total
                    mx[nb, nh] = highest
            if ahead is not None:
                result = jnp.max(top, axis=0, keepdims=True)
                return result if first else jnp.maximum(result, mx[b, h])
            return None

        def several(i, highest):
            for k in range(UNROLL):
                ahead = UNROLL * i + k + 1
                if k == UNROLL - 1:
                    ahead = jnp.minimum(ahead, items - 1)
                held, filled = (s0, s1) if k % 2 == 0 else (s1, s0)
                highest = step(ahead, filled, UNROLL * i + k, held, highest)
            return highest

        lax.fori_loop(0, items // UNROLL, several, step(0, s0, None, None, None))

    def share_column():
        each(zc_copy, GROUP, "wait_recv")
        zf[...] = zc[...].astype(F32).reshape(GROUP * 8, 128)
        for r in range(2):
            for j in range(4):
                coarse[column, r * 16:(r + 1) * 16, j * 128:(j + 1) * 128] = (
                    zf[pl.ds(2 * j + r, GROUP, stride=8), :].astype(BF16))
        each(coarse_copy, COLUMNS, "start")

    prepare(0, TOK, lambda r: near[BLOCK + r:BLOCK + r + PIECE, :], [(0, None, None)])
    attend(0, TOK, True, True, False)
    share_column()

    halo_copy(0).wait_recv()
    halo_copy(1).wait_recv()
    for b in range(2):
        beside = me * 2 + 3 * b - 1
        there = jnp.logical_and(beside >= 0, beside < all_blocks)
        prepare(TOK, BLOCK, lambda r, b=b: near[b * 3 * BLOCK + r:b * 3 * BLOCK + r + PIECE, :],
                [(b, lambda i, there=there: (i >= 0) & there, own_key(b))])
    attend(TOK, BLOCK, False, False, False)

    def prepare_mid(at_row, which):
        def usable_for(b):
            def usable(i):
                there = column * 32 + (i // 32 * 2 + which) * 2 + i // POOL % 2
                return jnp.abs(there - (me * 2 + b)) > 1
            return usable
        rows_at = lambda r: mid[which, r // 32:(r + PIECE) // 32].reshape(PIECE, 2 * KVW)
        prepare(at_row, MID // 2, rows_at, [(b, usable_for(b), own_key(b)) for b in range(2)])

    each(mid_copy, CHIPS, "wait_recv")
    relay.start()
    prepare_mid(0, core)
    relay.wait_recv()
    prepare_mid(MID // 2, 1 - core)
    attend(0, MID, False, False, False)

    each(coarse_copy, COLUMNS, "wait_recv")
    def usable_for(b):
        def usable(i):
            there = i // 32 * 32 + i % 16 * 2 + i // 16 % 2
            return (i // 32 != column) & (jnp.abs(there - (me * 2 + b)) > 1)
        return usable
    prepare(0, COARSE, lambda r: coarse[r // 32:(r + PIECE) // 32].reshape(PIECE, 2 * KVW),
            [(b, usable_for(b), own_key(b)) for b in range(2)])
    attend(0, COARSE, False, False, True)
    for b in range(2):
        out_ref[b * BLOCK:(b + 1) * BLOCK, :] = mixt[b].reshape(HEADS * HEAD_DIM, BLOCK).T

    each(zc_copy, GROUP, "wait_send")
    halo_copy(0).wait_send()
    halo_copy(1).wait_send()
    each(mid_copy, CHIPS, "wait_send")
    each(coarse_copy, COLUMNS, "wait_send")
    relay.wait_send()


def body(tokens, w_query, w_key, w_value, w_out):
    devices = lax.axis_size("seq")
    dma = pltpu.SemaphoreType.DMA
    mixed = pl.pallas_call(
        functools.partial(kernel, devices),
        out_shape=jax.ShapeDtypeStruct((TOK, D), BF16),
        in_specs=[pl.BlockSpec(memory_space=pltpu.HBM)] * 4,
        out_specs=pl.BlockSpec(memory_space=pltpu.VMEM),
        scratch_shapes=[
            pltpu.VMEM((TOK, D), BF16),
            pltpu.VMEM((D, 2 * KVW), BF16),
            pltpu.VMEM((D, HEADS * HEAD_DIM), BF16),
            pltpu.VMEM((4 * BLOCK, 2 * KVW), BF16),
            pltpu.VMEM((2, CHIPS, TOK // POOL, 2 * KVW), BF16),
            pltpu.VMEM((GROUP, 8, 128), BF16),
            pltpu.VMEM((GROUP * 8, 128), F32),
            pltpu.VMEM((COLUMNS, 32, 2 * KVW), BF16),
            pltpu.VMEM((2, HEADS, HEAD_DIM, BLOCK), BF16),
            pltpu.VMEM((2, KV_HEADS, NEAR, HEAD_DIM), BF16),
            pltpu.VMEM((2, KV_HEADS, VROWS, NEAR), BF16),
            pltpu.VMEM((TOK, BLOCK), F32),
            pltpu.VMEM((TOK, BLOCK), F32),
            pltpu.VMEM((2, HEADS, VROWS, BLOCK), F32),
            pltpu.VMEM((2, HEADS, 1, BLOCK), F32),
            pltpu.VMEM((2, HEADS, HEAD_DIM, BLOCK), BF16),
            dma((4,)),
            dma((2,)), dma((2,)),
            dma((CHIPS,)), dma((CHIPS,)),
            dma((GROUP,)), dma((GROUP,)),
            dma((COLUMNS,)), dma((COLUMNS,)),
            dma, dma,
        ],
        compiler_params=pltpu.CompilerParams(
            collective_id=0, has_side_effects=True, vmem_limit_bytes=40 * 1024 * 1024),
    )(*[pltpu.with_memory_space_constraint(x, pltpu.HBM) for x in (tokens, w_query, w_key, w_value)])
    return jnp.dot(mixed, w_out, preferred_element_type=F32).astype(BF16)


def solution(mesh):
    placed = (P("seq", None), P(), P(), P(), P())
    return jax.shard_map(
        body, mesh=mesh, in_specs=placed, out_specs=P("seq", None), check_vma=False
    )
```

```python
import functools
import math

import jax
import jax.numpy as jnp
from jax import lax
from jax.experimental import pallas as pl
from jax.experimental.pallas import tpu as pltpu
from jax.sharding import PartitionSpec as P

HEADS = 16
KV_HEADS = 4
PER_KV = HEADS // KV_HEADS
HEAD_DIM = 64
BLOCK = 256
POOL = 16
GROUP = 16
CHIPS = GROUP // 2
COLUMNS = 16
TOK = 512
UNROLL = 8
PIECE = 128
D = 1024
KVW = KV_HEADS * HEAD_DIM
NEAR = 3 * BLOCK
MID = 512
COARSE = 512
VROWS = HEAD_DIM + 16
C_EXP = math.log2(math.e) / math.sqrt(HEAD_DIM)
F32 = jnp.float32
BF16 = jnp.bfloat16
MESH = pl.DeviceIdType.MESH


def iota(shape, dim):
    return lax.broadcasted_iota(jnp.int32, shape, dim)


def dot(a, b):
    return jnp.dot(a, b, preferred_element_type=F32)


def kernel(devices, tok_hbm, wq_hbm, wk_hbm, wv_hbm, out_ref,
           tok, wkv, wq, near, mid, zc, zf, coarse, qt, kp, vt, s0, s1, acc, mx, mixt,
           load_sem, halo_s, halo_r, mid_s, mid_r, zc_s, zc_r, co_s, co_r, rel_s, rel_r):
    me = lax.axis_index("seq")
    core = lax.rem(me, 2)
    pos = lax.rem(me, GROUP)
    chip = lax.div(pos, 2)
    column = lax.div(me, GROUP)
    all_blocks = devices * 2

    def at(index):
        return (index,)

    loads = [
        pltpu.make_async_copy(tok_hbm, tok, load_sem.at[0]),
        pltpu.make_async_copy(wk_hbm, wkv.at[:, pl.ds(0, KVW)], load_sem.at[1]),
        pltpu.make_async_copy(wv_hbm, wkv.at[:, pl.ds(KVW, KVW)], load_sem.at[2]),
        pltpu.make_async_copy(wq_hbm, wq, load_sem.at[3]),
    ]
    for copy in loads:
        copy.start()

    def in_column(k):
        return column * GROUP + lax.rem(pos + k, GROUP)

    def across(k):
        return lax.rem(column + k, COLUMNS) * GROUP + pos

    following = lax.rem(me + 1, devices)
    previous = lax.rem(me + devices - 1, devices)
    partner = column * GROUP + chip * 2 + 1 - core

    barrier = pltpu.get_barrier_semaphore()

    def greet(k, _):
        pl.semaphore_signal(barrier, inc=1, device_id=at(in_column(k)), device_id_type=MESH)
        pl.semaphore_signal(barrier, inc=1, device_id=at(across(k)), device_id_type=MESH)
        return 0

    lax.fori_loop(1, GROUP, greet, 0)
    pl.semaphore_signal(barrier, inc=1, device_id=at(following), device_id_type=MESH)
    pl.semaphore_signal(barrier, inc=1, device_id=at(previous), device_id_type=MESH)

    for copy in loads[:3]:
        copy.wait()
    kv = dot(tok[...], wkv[...]).astype(BF16)
    near[pl.ds(BLOCK, TOK), :] = kv

    row, col = iota((32, TOK), 0), iota((32, TOK), 1)
    pool_mid = jnp.where(col // POOL == row, 1.0 / POOL, 0.0).astype(BF16)
    mid[core, chip] = dot(pool_mid, kv).astype(BF16)
    row, col = iota((16, TOK), 0), iota((16, TOK), 1)
    mine = jnp.zeros((16, 128), F32)
    for j in range(4):
        pool_coarse = jnp.where(col // BLOCK == row - 2 * j, 1.0 / BLOCK, 0.0).astype(BF16)
        mine += dot(pool_coarse, kv[:, j * 128:(j + 1) * 128])
    zc[pos] = mine[:8].astype(BF16)

    pl.semaphore_wait(barrier, 2 * GROUP)

    def zc_copy(k):
        return pltpu.make_async_remote_copy(
            src_ref=zc.at[pos], dst_ref=zc.at[pos], send_sem=zc_s.at[k], recv_sem=zc_r.at[k],
            device_id=at(in_column(k)), device_id_type=MESH)

    def halo_copy(which):
        src = near.at[pl.ds((2 - which) * BLOCK, BLOCK), :]
        dst = near.at[pl.ds(which * 3 * BLOCK, BLOCK), :]
        return pltpu.make_async_remote_copy(
            src_ref=src, dst_ref=dst, send_sem=halo_s.at[which], recv_sem=halo_r.at[which],
            device_id=at(previous if which else following), device_id_type=MESH)

    def mid_copy(k):
        target = column * GROUP + lax.rem(chip + k, CHIPS) * 2 + core
        return pltpu.make_async_remote_copy(
            src_ref=mid.at[core, chip], dst_ref=mid.at[core, chip],
            send_sem=mid_s.at[k], recv_sem=mid_r.at[k],
            device_id=at(target), device_id_type=MESH)

    def coarse_copy(k):
        return pltpu.make_async_remote_copy(
            src_ref=coarse.at[column], dst_ref=coarse.at[column],
            send_sem=co_s.at[k], recv_sem=co_r.at[k],
            device_id=at(across(k)), device_id_type=MESH)

    def each(copy_of, count, act):
        def step(k, _):
            getattr(copy_of(k), act)()
            return 0
        lax.fori_loop(1, count, step, 0)

    relay = pltpu.make_async_remote_copy(
        src_ref=mid.at[core], dst_ref=mid.at[core], send_sem=rel_s, recv_sem=rel_r,
        device_id=at(partner), device_id_type=MESH)

    each(zc_copy, GROUP, "start")
    halo_copy(0).start()
    halo_copy(1).start()
    each(mid_copy, CHIPS, "start")

    loads[3].wait()
    q = dot(tok[...], wq[...]).astype(BF16)
    for b in range(2):
        qt[b] = q[b * BLOCK:(b + 1) * BLOCK].T.reshape(HEADS, HEAD_DIM, BLOCK)

    def prepare(at_row, span, rows_at, variants):
        for r in range(0, span, PIECE):
            rows = rows_at(r)
            keys, values = rows[:, :KVW], rows[:, KVW:].T
            for slot, usable, own in variants:
                slot_keys, slot_values, count = keys, values, jnp.ones((16, PIECE), BF16)
                if usable is not None:
                    ok_rows = usable(iota((PIECE, 1), 0) + r)
                    ok_cols = usable(iota((1, PIECE), 1) + r)
                    slot_keys = jnp.where(ok_rows, keys.astype(F32), own).astype(BF16)
                    slot_values = jnp.where(ok_cols, values.astype(F32), 0.0).astype(BF16)
                    count = jnp.broadcast_to(jnp.where(ok_cols, 1.0, 0.0), (16, PIECE)).astype(BF16)
                there = pl.ds(at_row + r, PIECE)
                for kv_head in range(KV_HEADS):
                    part = slice(kv_head * HEAD_DIM, (kv_head + 1) * HEAD_DIM)
                    kp[slot, kv_head, there, :] = slot_keys[:, part]
                    vt[slot, kv_head, 0:HEAD_DIM, there] = slot_values[part]
                    vt[slot, kv_head, HEAD_DIM:VROWS, there] = count

    def own_key(b):
        return near[BLOCK + b * BLOCK:BLOCK + b * BLOCK + 16, :KVW].astype(F32)[0:1]

    def attend(base, span, shared, first, last):
        items = 2 * HEADS

        def place(i):
            b, h = lax.div(i, HEADS), lax.rem(i, HEADS)
            return b, h, (0 if shared else b), lax.div(h, PER_KV)

        def step(ahead, s_ahead, now, s_now, highest):
            if ahead is not None:
                b, h, slot, kv_head = place(ahead)
                query = qt[b, h]
                top = None
            if now is not None:
                nb, nh, nslot, nkv = place(now)
                total = None
            for t in range(0, span, BLOCK):
                if ahead is not None:
                    scores = dot(kp[slot, kv_head, base + t:base + t + BLOCK, :], query)
                    s_ahead[t:t + BLOCK, :] = scores
                    peak = jnp.max(scores.reshape(BLOCK // 8, 8, BLOCK), axis=0)
                    top = peak if top is None else jnp.maximum(top, peak)
                if now is not None:
                    weights = jnp.exp2((s_now[t:t + BLOCK, :] - highest) * C_EXP).astype(BF16)
                    part = dot(vt[nslot, nkv, :, base + t:base + t + BLOCK], weights)
                    total = part if total is None else total + part
            if now is not None:
                if not first:
                    total += acc[nb, nh] * jnp.exp2((mx[nb, nh] - highest) * C_EXP)
                if last:
                    inverse = 1.0 / total[HEAD_DIM:HEAD_DIM + 1]
                    mixt[nb, nh] = (total[:HEAD_DIM] * inverse).astype(BF16)
                else:
                    acc[nb, nh] = total
                    mx[nb, nh] = highest
            if ahead is not None:
                result = jnp.max(top, axis=0, keepdims=True)
                return result if first else jnp.maximum(result, mx[b, h])
            return None

        def several(i, highest):
            for k in range(UNROLL):
                ahead = UNROLL * i + k + 1
                if k == UNROLL - 1:
                    ahead = jnp.minimum(ahead, items - 1)
                held, filled = (s0, s1) if k % 2 == 0 else (s1, s0)
                highest = step(ahead, filled, UNROLL * i + k, held, highest)
            return highest

        lax.fori_loop(0, items // UNROLL, several, step(0, s0, None, None, None))

    def share_column():
        each(zc_copy, GROUP, "wait_recv")
        zf[...] = zc[...].astype(F32).reshape(GROUP * 8, 128)
        for r in range(2):
            for j in range(4):
                coarse[column, r * 16:(r + 1) * 16, j * 128:(j + 1) * 128] = (
                    zf[pl.ds(2 * j + r, GROUP, stride=8), :].astype(BF16))
        each(coarse_copy, COLUMNS, "start")

    prepare(0, TOK, lambda r: near[BLOCK + r:BLOCK + r + PIECE, :], [(0, None, None)])
    attend(0, TOK, True, True, False)
    share_column()

    def prepare_mid(at_row, which):
        def usable_for(b):
            def usable(i):
                there = column * 32 + (i // 32 * 2 + which) * 2 + i // POOL % 2
                return jnp.abs(there - (me * 2 + b)) > 1
            return usable
        rows_at = lambda r: mid[which, r // 32:(r + PIECE) // 32].reshape(PIECE, 2 * KVW)
        prepare(at_row, MID // 2, rows_at, [(b, usable_for(b), own_key(b)) for b in range(2)])

    each(mid_copy, CHIPS, "wait_recv")
    relay.start()
    prepare_mid(0, core)

    halo_copy(0).wait_recv()
    halo_copy(1).wait_recv()
    for b in range(2):
        beside = me * 2 + 3 * b - 1
        there = jnp.logical_and(beside >= 0, beside < all_blocks)
        prepare(TOK, BLOCK, lambda r, b=b: near[b * 3 * BLOCK + r:b * 3 * BLOCK + r + PIECE, :],
                [(b, lambda i, there=there: (i >= 0) & there, own_key(b))])

    relay.wait_recv()
    prepare_mid(MID // 2, 1 - core)
    attend(0, MID + BLOCK, False, False, False)

    each(coarse_copy, COLUMNS, "wait_recv")
    def usable_for(b):
        def usable(i):
            there = i // 32 * 32 + i % 16 * 2 + i // 16 % 2
            return (i // 32 != column) & (jnp.abs(there - (me * 2 + b)) > 1)
        return usable
    prepare(0, COARSE, lambda r: coarse[r // 32:(r + PIECE) // 32].reshape(PIECE, 2 * KVW),
            [(b, usable_for(b), own_key(b)) for b in range(2)])
    attend(0, COARSE, False, False, True)
    for b in range(2):
        out_ref[b * BLOCK:(b + 1) * BLOCK, :] = mixt[b].reshape(HEADS * HEAD_DIM, BLOCK).T

    each(zc_copy, GROUP, "wait_send")
    halo_copy(0).wait_send()
    halo_copy(1).wait_send()
    each(mid_copy, CHIPS, "wait_send")
    each(coarse_copy, COLUMNS, "wait_send")
    relay.wait_send()


def body(tokens, w_query, w_key, w_value, w_out):
    devices = lax.axis_size("seq")
    dma = pltpu.SemaphoreType.DMA
    mixed = pl.pallas_call(
        functools.partial(kernel, devices),
        out_shape=jax.ShapeDtypeStruct((TOK, D), BF16),
        in_specs=[pl.BlockSpec(memory_space=pltpu.HBM)] * 4,
        out_specs=pl.BlockSpec(memory_space=pltpu.VMEM),
        scratch_shapes=[
            pltpu.VMEM((TOK, D), BF16),
            pltpu.VMEM((D, 2 * KVW), BF16),
            pltpu.VMEM((D, HEADS * HEAD_DIM), BF16),
            pltpu.VMEM((4 * BLOCK, 2 * KVW), BF16),
            pltpu.VMEM((2, CHIPS, TOK // POOL, 2 * KVW), BF16),
            pltpu.VMEM((GROUP, 8, 128), BF16),
            pltpu.VMEM((GROUP * 8, 128), F32),
            pltpu.VMEM((COLUMNS, 32, 2 * KVW), BF16),
            pltpu.VMEM((2, HEADS, HEAD_DIM, BLOCK), BF16),
            pltpu.VMEM((2, KV_HEADS, NEAR, HEAD_DIM), BF16),
            pltpu.VMEM((2, KV_HEADS, VROWS, NEAR), BF16),
            pltpu.VMEM((NEAR, BLOCK), F32),
            pltpu.VMEM((NEAR, BLOCK), F32),
            pltpu.VMEM((2, HEADS, VROWS, BLOCK), F32),
            pltpu.VMEM((2, HEADS, 1, BLOCK), F32),
            pltpu.VMEM((2, HEADS, HEAD_DIM, BLOCK), BF16),
            dma((4,)),
            dma((2,)), dma((2,)),
            dma((CHIPS,)), dma((CHIPS,)),
            dma((GROUP,)), dma((GROUP,)),
            dma((COLUMNS,)), dma((COLUMNS,)),
            dma, dma,
        ],
        compiler_params=pltpu.CompilerParams(
            collective_id=0, has_side_effects=True, vmem_limit_bytes=40 * 1024 * 1024),
    )(*[pltpu.with_memory_space_constraint(x, pltpu.HBM) for x in (tokens, w_query, w_key, w_value)])
    return jnp.dot(mixed, w_out, preferred_element_type=F32).astype(BF16)


def solution(mesh):
    placed = (P("seq", None), P(), P(), P(), P())
    return jax.shard_map(
        body, mesh=mesh, in_specs=placed, out_specs=P("seq", None), check_vma=False
    )
```
